256 devices in a mesh: lat: 4 (over y_lo, core), lon: 64 (over y_hi, z, x).
Axes of the slice: x: 4, y: 4 (y_hi: 2, y_lo: 2; y = y_hi * 2 + y_lo), z: 8, core: 2. Of those that a mesh axis runs over, the one named last changes fastest.
Arguments:
- field: float32 [512, 1024, 128], P('lon', 'lat'), may hold values from -6 to 6
- kappa: float32 [512, 1024], P('lon', 'lat'), may hold values from 0.06 to 0.24
- classes: int32 [512, 1024], P('lon', 'lat'), may hold values from 0 to 7
- inverses: float32 [8, 128, 128], replicated, as said below
Outputs:
- result: float32 [512, 1024, 128], P('lon', 'lat')
The draws below stay inside these ranges and needn't reach their ends.
Inputs may be any that keep to these rules, and one draw needn't show every extreme that they name: `inverses`: each matrix has diagonal entries between 0.4 and 1.0 and dense, full-rank off-diagonal entries of magnitude about 0.02; the matrices are not diagonally dominant.
All inputs are finite; a program needn't handle non-finite values.
Results may differ from the reference program's by a relative error of at most 0.00013.
Values sent between devices are 32-bit elements; how exact they have to be, the bound alone decides.
No kernel may reach another device: no remote copies, remote signals or barrier semaphores. Data moves between devices by JAX's collectives and lax.ppermute only.
A program may use at most 64 MiB of HBM per device.

```python
import math
import jax
import jax.numpy as jnp
from jax import lax

LEV = 128
CLASSES = 8
STEPS = 6
NLON = 512
NLAT = 1024


def draw_inverses(key, part):
    key_diag = jax.random.fold_in(key, 11)
    key_off = jax.random.fold_in(key, 12)
    diag = jax.random.uniform(key_diag, (CLASSES, LEV), jnp.float32, 0.6, 1.0)
    off = 0.25 * jax.random.normal(key_off, (CLASSES, LEV, LEV), jnp.float32) / jnp.sqrt(jnp.float32(LEV))
    eye = jnp.eye(LEV, dtype=jnp.float32)
    return (off * (1.0 - eye) + diag[:, :, None] * eye).astype(jnp.float32)


def plant(entries, key, least, largest):
    place = [jax.random.randint(jax.random.fold_in(key, axis), (), 0, length) for axis, length in enumerate(entries.shape)]
    widest = entries.shape.index(max(entries.shape))
    beside = place[:widest] + [(place[widest] + 1) % entries.shape[widest]] + place[widest + 1:]
    return entries.at[tuple(place)].set(least).at[tuple(beside)].set(largest)


def block_levels(rng, dims, split, smallest, top_value):
    def one(position, blocks):
        heights = jax.random.uniform(jax.random.fold_in(jax.random.fold_in(rng, 6), position), (blocks,), jnp.float32, smallest / len(split), top_value / len(split))
        return jnp.repeat(jnp.exp(heights), dims[position] // blocks).reshape((-1,) + (1,) * (len(dims) - position - 1))

    loudness = one(*split[0])
    for cut in split[1:]:
        loudness = loudness * one(*cut)
    return loudness


def gaussian(own_key, extent, spread, reach, pieces=(), kind=jnp.bfloat16):
    array = jax.random.normal(own_key, extent, jnp.float32) * spread
    if len(pieces) > 0:
        array = block_levels(own_key, extent, pieces, -0.22, 0.18) * array
    return jnp.clip(array, min=-reach, max=reach).astype(kind)


def setup_inputs(seed: int = 0) -> dict:
    key_of = jax.random.split(jax.random.key(seed), 5)
    return {
        "field": gaussian(key_of[0], (NLON, NLAT, LEV), 1.0, 6.0, ((0, 64), (1, 4)), jnp.float32),
        "kappa": jnp.clip(jnp.exp(math.log(0.24) - 1.3862944 * jax.random.uniform(key_of[1], (NLON, NLAT), jnp.float32) ** block_levels(key_of[1], (NLON, NLAT), ((0, 64), (1, 4)), -0.2, 0.2)), 0.06, 0.24),
        "classes": plant(jax.random.randint(key_of[2], (NLON, NLAT), 0, CLASSES), jax.random.fold_in(key_of[2], 1), 0, CLASSES - 1).astype(jnp.int32),
        "inverses": draw_inverses(jax.random.fold_in(key_of[4], 71), 0),
    }


def explicit(field, kappa):
    east = jnp.roll(field, -1, 0)
    west = jnp.roll(field, 1, 0)
    k_east = jnp.roll(kappa, -1, 0)
    k_west = jnp.roll(kappa, 1, 0)
    padded = jnp.pad(field, ((0, 0), (1, 1), (0, 0)))
    k_padded = jnp.pad(kappa, ((0, 0), (1, 1)))
    north = padded[:, 2:]
    south = padded[:, :-2]
    k_north = k_padded[:, 2:]
    k_south = k_padded[:, :-2]
    total = (0.5 * (kappa + k_east))[..., None] * (east - field)
    total = total + (0.5 * (kappa + k_west))[..., None] * (west - field)
    total = total + (0.5 * (kappa + k_north))[..., None] * (north - field)
    total = total + (0.5 * (kappa + k_south))[..., None] * (south - field)
    return field + total


def vertical(field, classes, inverses):
    out = jnp.zeros(field.shape, jnp.float32)
    for kind in range(CLASSES):
        prod = jnp.einsum("xyl,ml->xym", field, inverses[kind], precision=lax.Precision.HIGHEST)
        out = out + jnp.where((classes == kind)[..., None], prod, jnp.float32(0.0))
    return out


def reference(field, kappa, classes, inverses):
    state = field
    for step in range(STEPS):
        state = vertical(explicit(state, kappa), classes, inverses)
    return state
```

```python
import jax
import jax.numpy as jnp
from jax import lax
from jax.experimental import pallas as pl
from jax.experimental.pallas import tpu as pltpu
from jax.sharding import PartitionSpec as P

STEPS = 6
NEAR = 4
FAR = STEPS - NEAR
PAD = 8
EDGE = 8
CHUNK = 16
BLOCK = 4
F32, BF16 = jnp.float32, jnp.bfloat16


def level_rows(near, before, lon):
    todo = []
    for s in range(1, STEPS + 1):
        low, high = s - near, lon - 1 + near - s
        if low > high:
            continue
        if before is not None and s - before <= lon - 1 + before - s:
            left = list(range(low, s - before))
            right = list(range(lon + before - s, high + 1))
            todo.append((s, left + right))
        else:
            todo.append((s, list(range(low, high + 1))))
    return todo


def place(keys, width, spare):
    return {key: spare + i * width for i, key in enumerate(keys)}


class Where:
    def __init__(self):
        self.at = {}

    def add(self, ref, table):
        for key, base in table.items():
            self.at[key] = (ref, base)

    def __getitem__(self, key):
        return self.at[key]


def spread(qt_ref, rows, width, outs):
    n = len(rows)
    q = qt_ref[...]
    k = lax.broadcasted_iota(jnp.int32, (128, 256), 0)
    lane = lax.broadcasted_iota(jnp.int32, (128, 256), 1)
    k5 = lax.rem(k, 5 * n)
    k5 = jnp.where(k < 15 * n, k5, -1)
    for name in range(5):
        ref, spare = outs[name]
        for i in range(0, n, 2):
            want = name * n + i + jnp.where(lane >= 128, 1, 0)
            one = jnp.where(k5 == want, 1.0, 0.0).astype(BF16)
            got = jnp.dot(q, one, preferred_element_type=F32)
            ref[pl.ds(spare + i * width, width), :] = got[:, :128].astype(ref.dtype)
            if i + 1 < n:
                ref[pl.ds(spare + (i + 1) * width, width), :] = got[:, 128:].astype(ref.dtype)


def advance(where, s, rows, width, lhs, wh, wl, emit):
    for first in range(0, len(rows), BLOCK):
        block = rows[first : first + BLOCK]
        for i, r in enumerate(block):
            cref, cb = where[("u", s - 1, r)]
            wref, wb = where[("u", s - 1, r - 1)]
            eref, eb = where[("u", s - 1, r + 1)]
            zref, zb = where[("c0", 0, r)]
            gref, gb = where[("fe", 0, r)]
            href, hb = where[("fe", 0, r - 1)]
            nref, nb = where[("fn", 0, r)]
            pref, pb = where[("pair", 0, r)]
            for j in range(0, width, CHUNK):
                d = lambda base: pl.ds(base + j, CHUNK)
                v = zref[d(zb), :] * cref[d(cb), :]
                v = v + gref[d(gb), :] * eref[d(eb), :]
                v = v + href[d(hb), :] * wref[d(wb), :]
                v = v + nref[d(nb), :] * cref[d(cb + 1), :]
                v = v + nref[d(nb - 1), :] * cref[d(cb - 1), :]
                high = v.astype(BF16)
                low = (v - high.astype(F32)).astype(BF16)
                kind = pref[d(pb), :]
                zero = jnp.zeros_like(high)
                here = pl.ds(i * width + j, CHUNK)
                for q in range(4):
                    hit = kind == jnp.asarray(q, BF16)
                    lhs[here, q * 128 : (q + 1) * 128] = jnp.where(hit, high, zero)
                    lhs[here, 512 + q * 128 : 640 + q * 128] = jnp.where(hit, low, zero)
        m = len(block) * width
        high = lhs[pl.ds(0, m), 0:512]
        low = lhs[pl.ds(0, m), 512:1024]
        got = jnp.dot(high, wh[...], preferred_element_type=F32)
        got = got + jnp.dot(high, wl[...], preferred_element_type=F32)
        got = got + jnp.dot(low, wh[...], preferred_element_type=F32)
        for i, r in enumerate(block):
            oref, ob = where[("odd", 0, r)]
            piece = got[i * width : (i + 1) * width]
            odd = oref[pl.ds(ob, width), :]
            emit(s, r, jnp.where(odd > 0.5, piece[:, 128:], piece[:, :128]))


NAMES = ("c0", "fe", "fn", "odd", "pair")


def add_coefs(where, refs, tables):
    for name, ref in zip(NAMES, refs):
        where.add(ref, tables[name])


def coef_tables(rows, fe_rows, width):
    out = {}
    for name in NAMES:
        spare = 0 if name == "pair" else EDGE
        out[name] = place([(name, 0, r) for r in (fe_rows if name == "fe" else rows)], width, spare)
    return out


def coef_shapes(n, width):
    flat = [jax.ShapeDtypeStruct((n * width + 2 * EDGE, 128), F32)] * 4
    return flat + [jax.ShapeDtypeStruct((n * width, 128), BF16)]


def coef_outs(refs):
    return [(ref, EDGE) for ref in refs[:4]] + [(refs[4], 0)]


def call(kernel, ins, outs, scratch, flops, name):
    vmem = pl.BlockSpec(memory_space=pltpu.VMEM)
    return pl.pallas_call(
        kernel,
        out_shape=outs,
        in_specs=[vmem] * len(ins),
        out_specs=[vmem] * len(outs),
        scratch_shapes=scratch,
        compiler_params=pltpu.CompilerParams(vmem_limit_bytes=20 << 20),
        cost_estimate=pl.CostEstimate(flops=flops, bytes_accessed=1 << 20, transcendentals=0),
        name=name,
    )(*ins)


def body(field, kappa, classes, inverses):
    lon, lats, lev = field.shape
    width = lats + 2 * PAD
    n_lon, n_lat = lax.axis_size("lon"), lax.axis_size("lat")
    east = [(i, (i + 1) % n_lon) for i in range(n_lon)]
    west = [(j, i) for i, j in east]
    north = [(i, (i + 1) % n_lat) for i in range(n_lat)]
    south = [(j, i) for i, j in north]
    lat = lax.axis_index("lat")
    kinds = classes.astype(F32)

    per = lats // 128
    meta = jnp.concatenate(
        [kappa.reshape(lon, per, 128), kinds.reshape(lon, per, 128), jnp.zeros((lon, 8 - 2 * per, 128), F32)], axis=1
    )

    def rows_of(lo, hi):
        return jnp.concatenate([field[lo:hi], meta[lo:hi]], axis=1)

    def cols_of(lo, hi):
        line = jnp.concatenate(
            [kappa[:, lo:hi], kinds[:, lo:hi], jnp.zeros((lon, 128 - 2 * STEPS), F32)], axis=1
        )
        return jnp.concatenate([field[:, lo:hi], line[:, None], jnp.zeros((lon, 1, 128), F32)], axis=1)

    to_north, to_south = cols_of(lats - STEPS, lats), cols_of(0, STEPS)
    from_south = lax.ppermute(to_north, "lat", north)
    from_north = lax.ppermute(to_south, "lat", south)
    from_west = lax.ppermute(rows_of(lon - NEAR, lon), "lon", east)
    from_east = lax.ppermute(rows_of(0, NEAR), "lon", west)
    from_south = from_south * jnp.where(lat > 0, 1.0, 0.0).astype(F32)
    from_north = from_north * jnp.where(lat < n_lat - 1, 1.0, 0.0).astype(F32)
    corners = jnp.concatenate([from_south, from_north], axis=1)
    corner_west = lax.ppermute(corners[lon - STEPS :], "lon", east)
    corner_east = lax.ppermute(corners[:STEPS], "lon", west)
    far_west = lax.ppermute(rows_of(lon - STEPS, lon - NEAR), "lon", east)
    far_east = lax.ppermute(rows_of(NEAR, STEPS), "lon", west)

    def line_of(middle, sides, which):
        a, b = which * STEPS, (which + 1) * STEPS
        zero = jnp.zeros((middle.shape[0], PAD - STEPS), F32)
        return jnp.concatenate([zero, sides[:, STEPS, a:b], middle, sides[:, 8 + STEPS, a:b], zero], axis=1)

    def lines_of(message, sides):
        n = message.shape[0]
        mk = message[:, lats : lats + per].reshape(n, lats)
        mc = message[:, lats + per : lats + 2 * per].reshape(n, lats)
        return line_of(mk, sides, 0), line_of(mc, sides, 1)

    k_own, c_own = line_of(kappa, corners, 0), line_of(kinds, corners, 1)
    kw, cw = lines_of(from_west, corner_west[FAR:])
    ke, ce = lines_of(from_east, corner_east[:NEAR])
    kfw, cfw = lines_of(far_west, corner_west[:FAR])
    kfe, cfe = lines_of(far_east, corner_east[NEAR:])
    place_lat = lat * lats + jnp.arange(width, dtype=jnp.int32) - PAD
    inside = ((place_lat >= 0) & (place_lat < lats * n_lat)).astype(F32)
    both = inside * jnp.concatenate([inside[1:], jnp.zeros((1,), F32)])

    def numbers(k, c, start, rows, fe_rows):
        fe = 0.5 * (k[:-1] + k[1:])
        fn = 0.5 * (k + jnp.concatenate([k[:, 1:], jnp.zeros_like(k[:, :1])], axis=1))
        fs = jnp.concatenate([jnp.zeros_like(k[:, :1]), fn[:, :-1]], axis=1)
        zero = jnp.zeros_like(k[:1])
        c0 = 1.0 - jnp.concatenate([fe, zero]) - jnp.concatenate([zero, fe]) - fn - fs
        pair = jnp.floor(c * 0.5)
        odd = c - 2.0 * pair

        def take(a, which):
            runs, i = [], 0
            while i < len(which):
                j = i
                while j + 1 < len(which) and which[j + 1] == which[j] + 1:
                    j += 1
                runs.append(a[which[i] - start : which[j] - start + 1])
                i = j + 1
            return jnp.concatenate(runs) if len(runs) > 1 else runs[0]

        q = jnp.concatenate(
            [
                take(c0 * inside, rows),
                take(fe * inside, fe_rows),
                take(fn * both, rows),
                take(odd, rows),
                take(pair, rows),
            ]
        )
        high = lax.reduce_precision(q, 8, 7)
        mid = lax.reduce_precision(q - high, 8, 7)
        low = q - high - mid
        all3 = jnp.concatenate([high, mid, low, jnp.zeros((128 - 3 * q.shape[0], width), F32)])
        return all3.T.astype(BF16)

    rows_a = list(range(0, lon - 1))
    rows_b = list(range(1 - NEAR, 1)) + list(range(lon - 1, lon - 1 + NEAR))
    fe_b = list(range(-NEAR, 0)) + list(range(lon - 1, lon - 1 + NEAR))
    rows_c = list(range(1 - STEPS, 1 - NEAR)) + list(range(lon - 1 + NEAR, lon - 1 + STEPS))
    fe_c = list(range(-STEPS, -NEAR)) + list(range(lon - 1 + NEAR, lon - 1 + STEPS))
    q_a = numbers(k_own, c_own, 0, rows_a, rows_a)
    k_b, c_b = jnp.concatenate([kw, k_own, ke]), jnp.concatenate([cw, c_own, ce])
    q_b = numbers(k_b, c_b, -NEAR, rows_b, fe_b)
    k_c, c_c = jnp.concatenate([kfw, k_b, kfe]), jnp.concatenate([cfw, c_b, cfe])
    q_c = numbers(k_c, c_c, -STEPS, rows_c, fe_c)
    tab_a = coef_tables(rows_a, rows_a, width)
    tab_b = coef_tables(rows_b, fe_b, width)
    tab_c = coef_tables(rows_c, fe_c, width)

    kinds_n = inverses.shape[0]
    w = inverses.reshape(kinds_n // 2, 2, lev, lev).transpose(0, 3, 1, 2).reshape(kinds_n // 2 * lev, 2 * lev)

    todo_a = level_rows(0, None, lon)
    todo_b = level_rows(NEAR, 0, lon)
    todo_c = level_rows(STEPS, NEAR, lon)
    keys_a = [("u", 0, r) for r in range(lon)] + [("u", s, r) for s, rs in todo_a for r in rs]
    keys_b = [("u", 0, r) for r in list(range(-NEAR, 0)) + list(range(lon, lon + NEAR))]
    keys_b += [("u", s, r) for s, rs in todo_b for r in rs if s < STEPS]
    keys_c = [("u", 0, r) for r in list(range(-STEPS, -NEAR)) + list(range(lon + NEAR, lon + STEPS))]
    keys_c += [("u", s, r) for s, rs in todo_c for r in rs if s < STEPS]
    at_a, at_b, at_c = place(keys_a, width, EDGE), place(keys_b, width, EDGE), place(keys_c, width, EDGE)
    done_b = [r for s, rs in todo_b if s == STEPS for r in rs]
    lhs = pltpu.VMEM((BLOCK * width, 1024), BF16)

    def flat(keys):
        return jax.ShapeDtypeStruct((len(keys) * width + 2 * EDGE, 128), F32)

    def load_row(ref, base, middle, first, last):
        ref[pl.ds(base, PAD), :] = jnp.zeros((PAD, 128), F32)
        ref[pl.ds(base + width - PAD, PAD), :] = jnp.zeros((PAD, 128), F32)
        ref[pl.ds(base + PAD - STEPS, STEPS), :] = first
        ref[pl.ds(base + PAD, lats), :] = middle
        ref[pl.ds(base + PAD + lats, STEPS), :] = last

    def flops(todo):
        return sum(len(rs) for _, rs in todo) * width * 1536 * 256 * 2

    def kernel_a(field_ref, side_ref, qt_ref, w_ref, u_ref, c0, fe, fn, odd, pair, wh, wl, left):
        wf = w_ref[...]
        hi = wf.astype(BF16)
        wh[...] = hi
        wl[...] = (wf - hi.astype(F32)).astype(BF16)
        coefs = (c0, fe, fn, odd, pair)
        spread(qt_ref, rows_a, width, coef_outs(coefs))
        for r in range(lon):
            load_row(u_ref, at_a[("u", 0, r)], field_ref[r], side_ref[r, 0:STEPS], side_ref[r, 8 : 8 + STEPS])
        where = Where()
        where.add(u_ref, at_a)
        add_coefs(where, coefs, tab_a)

        def emit(s, r, x):
            u_ref[pl.ds(at_a[("u", s, r)], width), :] = x

        for s, rs in todo_a:
            advance(where, s, rs, width, left, wh, wl, emit)

    outs_a = [flat(keys_a)] + coef_shapes(len(rows_a), width) + [jax.ShapeDtypeStruct(w.shape, BF16)] * 2
    res_a = call(kernel_a, (field, corners, q_a, w), outs_a, [lhs], flops(todo_a), "inner")
    u_a, coef_a, wh, wl = res_a[0], res_a[1:6], res_a[6], res_a[7]

    def kernel_b(*refs):
        near_w, near_e, cor_w, cor_e, qt_ref, ua, *rest = refs
        ca, (wh_r, wl_r, ub, *cb), (done, left) = rest[:5], rest[5:13], rest[13:]
        spread(qt_ref, rows_b, width, coef_outs(cb))
        for i in range(NEAR):
            base = at_b[("u", 0, i - NEAR)]
            load_row(ub, base, near_w[i, 0:lats], cor_w[FAR + i, 0:STEPS], cor_w[FAR + i, 8 : 8 + STEPS])
            base = at_b[("u", 0, lon + i)]
            load_row(ub, base, near_e[i, 0:lats], cor_e[i, 0:STEPS], cor_e[i, 8 : 8 + STEPS])
        where = Where()
        where.add(ua, at_a)
        add_coefs(where, ca, tab_a)
        where.add(ub, at_b)
        add_coefs(where, cb, tab_b)

        def emit(s, r, x):
            if s == STEPS:
                done[done_b.index(r)] = x[PAD : PAD + lats]
            else:
                ub[pl.ds(at_b[("u", s, r)], width), :] = x

        for s, rs in todo_b:
            advance(where, s, rs, width, left, wh_r, wl_r, emit)

    outs_b = [flat(keys_b)] + coef_shapes(len(rows_b), width)
    outs_b += [jax.ShapeDtypeStruct((len(done_b), lats, lev), F32)]
    ins_b = (from_west, from_east, corner_west, corner_east, q_b, u_a, *coef_a, wh, wl)
    res_b = call(kernel_b, ins_b, outs_b, [lhs], flops(todo_b), "middle")
    u_b, coef_b, done = res_b[0], res_b[1:6], res_b[6]

    def kernel_c(*refs):
        far_w, far_e, cor_w, cor_e, qt_ref, ua, ub, *rest = refs
        ca, cb, (wh_r, wl_r, done_ref, out), (uc, *cc) = rest[:5], rest[5:10], rest[10:14], rest[14:20]
        left = rest[20]
        for i, r in enumerate(done_b):
            out[r] = done_ref[i]
        spread(qt_ref, rows_c, width, coef_outs(cc))
        for i in range(FAR):
            base = at_c[("u", 0, i - STEPS)]
            load_row(uc, base, far_w[i, 0:lats], cor_w[i, 0:STEPS], cor_w[i, 8 : 8 + STEPS])
            base = at_c[("u", 0, lon + NEAR + i)]
            load_row(uc, base, far_e[i, 0:lats], cor_e[NEAR + i, 0:STEPS], cor_e[NEAR + i, 8 : 8 + STEPS])
        where = Where()
        for ref, at in ((ua, at_a), (ub, at_b), (uc, at_c)):
            where.add(ref, at)
        for refs_, tab in ((ca, tab_a), (cb, tab_b), (cc, tab_c)):
            add_coefs(where, refs_, tab)

        def emit(s, r, x):
            if s == STEPS:
                out[r] = x[PAD : PAD + lats]
            else:
                uc[pl.ds(at_c[("u", s, r)], width), :] = x

        for s, rs in todo_c:
            advance(where, s, rs, width, left, wh_r, wl_r, emit)

    scratch = [pltpu.VMEM(x.shape, x.dtype) for x in [flat(keys_c)] + coef_shapes(len(rows_c), width)] + [lhs]
    ins_c = (far_west, far_east, corner_west, corner_east, q_c, u_a, u_b, *coef_a, *coef_b, wh, wl, done)
    (out,) = call(kernel_c, ins_c, [jax.ShapeDtypeStruct(field.shape, F32)], scratch, flops(todo_c), "outer")
    return out


def solution(mesh):
    return jax.shard_map(
        body,
        mesh=mesh,
        in_specs=(P("lon", "lat", None), P("lon", "lat"), P("lon", "lat"), P()),
        out_specs=P("lon", "lat", None),
        check_vma=False,
    )
```

```python
import jax
import jax.numpy as jnp
from jax import lax
from jax.experimental import pallas as pl
from jax.experimental.pallas import tpu as pltpu
from jax.sharding import PartitionSpec as P

STEPS = 6
NEAR = 3
FAR = STEPS - NEAR
PAD = 8
EDGE = 8
F32, BF16 = jnp.float32, jnp.bfloat16


def level_rows(near, before, lon):
    todo = []
    for s in range(1, STEPS + 1):
        low, high = s - near, lon - 1 + near - s
        if low > high:
            continue
        if before is not None and s - before <= lon - 1 + before - s:
            todo.append((s, list(range(low, s - before)), list(range(lon + before - s, high + 1))))
        else:
            todo.append((s, list(range(low, high + 1)), []))
    return todo


def blocks_of(todo):
    out = []
    for s, left, right in todo:
        rows = left + right
        out += [(s, rows[i], rows[i + 1]) for i in range(0, len(rows), 2)]
    return out


def place(keys, width):
    return {key: EDGE + i * width for i, key in enumerate(keys)}


class Where:
    def __init__(self):
        self.at = {}

    def add(self, ref, table):
        for key, base in table.items():
            self.at[key] = (ref, base)

    def __getitem__(self, key):
        return self.at[key]


def pack_rows(ref, first, field, k, c, lats):
    for i in range(ref.shape[0]):
        r = first + i
        ref[i, 0:lats] = field[r]
        ref[i, lats : lats + 8] = jnp.zeros((8, 128), F32)
        for h in range(lats // 128):
            at = lats + h
            ref[i, at : at + 1] = k[r : r + 1, h * 128 : (h + 1) * 128]
            at = lats + lats // 128 + h
            ref[i, at : at + 1] = c[r : r + 1, h * 128 : (h + 1) * 128]


def pack_kernel(lon, lats):
    def kernel(field, small, to_north, to_south, near_e, near_w):
        k, c = small[0:lon], small[lon : 2 * lon]
        lane = lax.broadcasted_iota(jnp.int32, (lon, 128), 1)
        k_first, k_last = k[:, :128], k[:, lats - 128 :]
        c_first, c_last = c[:, :128], c[:, lats - 128 :]
        line_n = jnp.where(lane < 64, pltpu.roll(k_last, 8, 1), pltpu.roll(c_last, 72, 1))
        line_s = jnp.where(lane < 64, k_first, pltpu.roll(c_first, 64, 1))
        for r in range(lon):
            to_north[r] = field[r, lats - 8 : lats]
            to_north[r, 0:1] = line_n[r : r + 1]
            to_south[r] = field[r, 0:8]
            to_south[r, 7:8] = line_s[r : r + 1]

        pack_rows(near_e, lon - NEAR, field, k, c, lats)
        pack_rows(near_w, 0, field, k, c, lats)

    return kernel


def corner_kernel(lon, lats):
    def kernel(from_south, from_north, field, small, corners, corner_e, corner_w, far_e, far_w):
        k, c = small[0:lon], small[lon : 2 * lon]
        pack_rows(far_e, lon - STEPS, field, k, c, lats)
        pack_rows(far_w, NEAR, field, k, c, lats)
        lat = lax.axis_index("lat")
        n_lat = lax.axis_size("lat")
        has_s = jnp.where(lat > 0, 1.0, 0.0).astype(F32)
        has_n = jnp.where(lat < n_lat - 1, 1.0, 0.0).astype(F32)
        for r in range(lon):
            s, n = from_south[r] * has_s, from_north[r] * has_n
            corners[r, 0:8] = s
            corners[r, 8:16] = n
            if r >= lon - STEPS:
                corner_e[r - (lon - STEPS), 0:8] = s
                corner_e[r - (lon - STEPS), 8:16] = n
            if r < STEPS:
                corner_w[r, 0:8] = s
                corner_w[r, 8:16] = n

    return kernel


def split3(x):
    high = x.astype(BF16).astype(F32)
    mid = (x - high).astype(BF16).astype(F32)
    return [high, mid, x - high - mid]


def spread(lines, kinds, sides, rows_at, kb, pair, odd, lats, width):
    k = lax.broadcasted_iota(jnp.int32, (32, 256), 0)
    lane = lax.broadcasted_iota(jnp.int32, (32, 256), 1)
    dims = (((0,), (0,)), ((), ()))

    def put(at, n, value):
        half = jnp.floor(value * 0.5)
        pair[pl.ds(at, n), :] = half
        odd[pl.ds(at, n), :] = value - 2.0 * half

    mine = lax.rem(k, 8)
    full = [jnp.concatenate(split3(a) + [c]).astype(BF16) for a, c in zip(lines, kinds)]
    edge = [jnp.concatenate(split3(a) + [jnp.zeros((8, 128), F32)]).astype(BF16) for a in sides]
    for i, at in enumerate(rows_at):
        hit = (mine == i) & ((k >= 24) == (lane >= 128))
        one = jnp.where(hit, 1.0, 0.0).astype(BF16)
        for h, x in enumerate(full):
            got = lax.dot_general(x, one, dims, preferred_element_type=F32)
            here = at + PAD + h * 128
            kb[pl.ds(here, 128), :] = got[:, :128]
            put(here, 128, got[:, 128:])
        for x, here in zip(edge, (at, at + PAD + lats)):
            got = lax.dot_general(x, one, dims, preferred_element_type=F32)
            kb[pl.ds(here, 8), :] = got[0:8, :128]
            put(here, 8, got[64:72, :128])


def load_row(ref, base, middle, sides, lats):
    sub = lax.broadcasted_iota(jnp.int32, (8, 128), 0)
    ref[pl.ds(base, 8), :] = jnp.where(sub == 0, 0.0, sides[0:8])
    ref[pl.ds(base + PAD, lats), :] = middle
    ref[pl.ds(base + PAD + lats, 8), :] = jnp.where(sub == 7, 0.0, sides[8:16])


def faces(where, rows, fe_rows, width):
    for r in fe_rows:
        a, ab = where[("kb", 0, r)]
        b, bb = where[("kb", 0, r + 1)]
        o, ob = where[("fe", 0, r)]
        for j in range(0, width, 8):
            o[pl.ds(ob + j, 8), :] = 0.5 * (a[pl.ds(ab + j, 8), :] + b[pl.ds(bb + j, 8), :])
    for r in rows:
        k, kb = where[("kb", 0, r)]
        e, eb = where[("fe", 0, r)]
        w, wb = where[("fe", 0, r - 1)]
        z, zb = where[("c0", 0, r)]
        n, nb = where[("fn", 0, r)]
        for j in range(0, width, 8):
            mid = k[pl.ds(kb + j, 8), :]
            up = k[pl.ds(kb + j + 1, 8), :]
            fn = 0.5 * (mid + up)
            fs = 0.5 * (mid + k[pl.ds(kb + j - 1, 8), :])
            c0 = 1.0 - e[pl.ds(eb + j, 8), :] - w[pl.ds(wb + j, 8), :] - fn - fs
            z[pl.ds(zb + j, 8), :] = jnp.where(mid > 0.0, c0, 0.0)
            n[pl.ds(nb + j, 8), :] = jnp.where((mid > 0.0) & (up > 0.0), fn, 0.0)


def advance(where, blocks, width, wh, wl, v, vl, emit, accs):
    def explicit(b):
        s, *rows = blocks[b]
        for q, r in enumerate(rows):
            cref, cb = where[("u", s - 1, r)]
            wref, wb = where[("u", s - 1, r - 1)]
            eref, eb = where[("u", s - 1, r + 1)]
            zref, zb = where[("c0", 0, r)]
            gref, gb = where[("fe", 0, r)]
            href, hb = where[("fe", 0, r - 1)]
            nref, nb = where[("fn", 0, r)]
            for j in range(0, width, 8):
                d = lambda base: pl.ds(base + j, 8)
                x = zref[d(zb), :] * cref[d(cb), :]
                x = x + gref[d(gb), :] * eref[d(eb), :]
                x = x + href[d(hb), :] * wref[d(wb), :]
                x = x + nref[d(nb), :] * cref[d(cb + 1), :]
                x = x + nref[d(nb - 1), :] * cref[d(cb - 1), :]
                v[b % 2, q, j : j + 8] = x
                vl[b % 2, q, j : j + 8] = x - x.astype(BF16).astype(F32)

    tiles = [(x, w, t) for t in range(2) for x, w in ((v, wh), (v, wl), (vl, wh))]

    def push(k):
        _, w, t = tiles[k]
        for q in range(2):
            pltpu.matmul_push_rhs(w[t * 256 : (t + 1) * 256, :], staging_register=k % 2, mxu_index=q)

    def products(b):
        _, *rows = blocks[b]
        push(0)
        for k, (x, _, t) in enumerate(tiles):
            if k + 1 < len(tiles):
                push(k + 1)
            for q, r in enumerate(rows):
                pref, pb = where[("pair", 0, r)]
                pair = pref[pl.ds(pb, width), :]
                value = x[b % 2, q]
                lhs = [jnp.where(pair == float(2 * t + i), value, 0.0) for i in range(2)]
                pltpu.matmul_acc_lhs(accs[q][b % 2], jnp.concatenate(lhs, axis=1), load_staged_rhs=k % 2)

    def finish(b):
        s, *rows = blocks[b]
        for q, r in enumerate(rows):
            got = pltpu.matmul_pop(accs[q][b % 2])
            oref, ob = where[("odd", 0, r)]
            odd = oref[pl.ds(ob, width), :]
            emit(s, r, jnp.where(odd > 0.5, got[:, 128:], got[:, :128]))

    for b, (s, *rows) in enumerate(blocks):
        need = {r + d for r in rows for d in (-1, 0, 1)}
        wait = b > 0 and blocks[b - 1][0] == s - 1 and bool(need & set(blocks[b - 1][1:]))
        if wait:
            finish(b - 1)
        explicit(b)
        products(b)
        if b > 0 and not wait:
            finish(b - 1)
    finish(len(blocks) - 1)


def call(kernel, ins, outs, scratch, name, flops=0, limit=8 << 20):
    vmem = pl.BlockSpec(memory_space=pltpu.VMEM)
    return pl.pallas_call(
        kernel,
        out_shape=outs,
        in_specs=[vmem] * len(ins),
        out_specs=[vmem] * len(outs),
        scratch_shapes=scratch,
        compiler_params=pltpu.CompilerParams(vmem_limit_bytes=limit),
        cost_estimate=pl.CostEstimate(flops=flops, bytes_accessed=1 << 20, transcendentals=0),
        name=name,
    )(*ins)


def body(field, kappa, classes, inverses):
    lon, lats, lev = field.shape
    width = lats + 2 * PAD
    n_lon, n_lat = lax.axis_size("lon"), lax.axis_size("lat")
    east = [(i, (i + 1) % n_lon) for i in range(n_lon)]
    west = [(j, i) for i, j in east]
    north = [(i, (i + 1) % n_lat) for i in range(n_lat)]
    south = [(j, i) for i, j in north]
    halves = lats // 128

    def arr(*shape, dtype=F32):
        return jax.ShapeDtypeStruct(shape, dtype)

    def flat(n):
        return arr(n * width + 2 * EDGE, 128)

    edge, near, far, corner = (lon, 8, 128), (NEAR, lats + 8, 128), (FAR, lats + 8, 128), (STEPS, 16, 128)
    small = jnp.concatenate([kappa, classes.astype(F32)])
    to_north, to_south, near_e, near_w = call(
        pack_kernel(lon, lats), (field, small), [arr(*x) for x in (edge, edge, near, near)], [], "pack"
    )
    from_south = lax.ppermute(to_north, "lat", north)
    from_north = lax.ppermute(to_south, "lat", south)
    from_west = lax.ppermute(near_e, "lon", east)
    from_east = lax.ppermute(near_w, "lon", west)
    corners, corner_e, corner_w, far_e, far_w = call(
        corner_kernel(lon, lats),
        (from_south, from_north, field, small),
        [arr(lon, 16, 128), arr(*corner), arr(*corner), arr(*far), arr(*far)],
        [],
        "corner",
    )
    corner_west = lax.ppermute(corner_e, "lon", east)
    corner_east = lax.ppermute(corner_w, "lon", west)
    far_west = lax.ppermute(far_e, "lon", east)
    far_east = lax.ppermute(far_w, "lon", west)

    todo_a, todo_b, todo_c = level_rows(0, None, lon), level_rows(NEAR, 0, lon), level_rows(STEPS, NEAR, lon)

    def later(todo, last):
        return [("u", s, r) for s, a, b in todo for r in a + b if s < last]

    own = list(range(lon))
    halo_b = list(range(-NEAR, 0)) + list(range(lon, lon + NEAR))
    halo_c = list(range(-STEPS, -NEAR)) + list(range(lon + NEAR, lon + STEPS))
    rows_a, fe_a = own[1:-1], own[:-1]
    rows_b = list(range(1 - NEAR, 1)) + list(range(lon - 1, lon - 1 + NEAR))
    fe_b = list(range(-NEAR, 0)) + list(range(lon - 1, lon - 1 + NEAR))
    rows_c = list(range(1 - STEPS, 1 - NEAR)) + list(range(lon - 1 + NEAR, lon - 1 + STEPS))
    fe_c = list(range(-STEPS, -NEAR)) + list(range(lon - 1 + NEAR, lon - 1 + STEPS))

    def at0(name, rows):
        return place([(name, 0, r) for r in rows], width)

    def phase_tables(halo, rows, fe_rows):
        names = [("u", halo), ("kb", halo), ("pair", halo), ("odd", halo), ("c0", rows), ("fe", fe_rows), ("fn", rows)]
        return [(len(rs), at0(name, rs)) for name, rs in names]

    tabs_a = phase_tables(own, rows_a, fe_a)
    tabs_b = phase_tables(halo_b, rows_b, fe_b)
    tabs_c = phase_tables(halo_c, rows_c, fe_c)

    def shapes(tabs):
        return [flat(n) for n, _ in tabs]

    def found(*pairs):
        where = Where()
        for refs, tabs in pairs:
            for ref, (_, table) in zip(refs, tabs):
                where.add(ref, table)
        return where

    def msg_lines(ref_rows, which):
        out = []
        for h in range(halves):
            at = lats + which * halves + h
            rows = [ref[i, at : at + 1] for ref, i in ref_rows]
            rows += [jnp.zeros((8 - len(rows), 128), F32)] * (len(rows) < 8)
            out.append(jnp.concatenate(rows))
        return out

    def side_lines(ref_rows):
        out = []
        for at in (0, 15):
            rows = [ref[i, at : at + 1] for ref, i in ref_rows]
            rows += [jnp.zeros((8 - len(rows), 128), F32)] * (len(rows) < 8)
            out.append(jnp.concatenate(rows))
        return out

    def setup_a(field_ref, small_ref, corners_ref, inv_ref, u, kb, pair, odd, c0, fe, fn, wh, wl):
        for kind in range(inv_ref.shape[0]):
            w = inv_ref[kind].T
            high = w.astype(BF16)
            here = (slice((kind // 2) * lev, (kind // 2 + 1) * lev), slice((kind % 2) * lev, (kind % 2 + 1) * lev))
            wh[here] = high
            wl[here] = (w - high.astype(F32)).astype(BF16)
        k, c = small_ref[0:lon], small_ref[lon : 2 * lon]
        lines = [k[:, h * 128 : (h + 1) * 128] for h in range(halves)]
        kinds = [c[:, h * 128 : (h + 1) * 128] for h in range(halves)]
        at = tabs_a[1][1]
        sides = side_lines([(corners_ref, r) for r in own])
        spread(lines, kinds, sides, [at[("kb", 0, r)] for r in own], kb, pair, odd, lats, width)
        for r in own:
            load_row(u, tabs_a[0][1][("u", 0, r)], field_ref[r], corners_ref[r], lats)
        faces(found(((u, kb, pair, odd, c0, fe, fn), tabs_a)), rows_a, fe_a, width)

    pairs_n = inverses.shape[0] // 2
    weights = arr(pairs_n * lev, 2 * lev, dtype=BF16)
    *set_a, wh, wl = call(
        setup_a, (field, small, corners, inverses), shapes(tabs_a) + [weights] * 2, [], "own"
    )

    def setup_halo(tabs, earlier, halo, rows, fe_rows, corner_of):
        half = len(halo) // 2

        def kernel(*refs):
            w_ref, e_ref, cw_ref, ce_ref, *rest = refs
            before, outs = rest[: len(earlier)], rest[len(earlier) :]
            u, kb, pair, odd, c0, fe, fn = outs
            msgs = [(w_ref, i) for i in range(half)] + [(e_ref, i) for i in range(half)]
            cors = [(cw_ref, corner_of[0] + i) for i in range(half)] + [(ce_ref, corner_of[1] + i) for i in range(half)]
            at = [tabs[1][1][("kb", 0, r)] for r in halo]
            spread(msg_lines(msgs, 0), msg_lines(msgs, 1), side_lines(cors), at, kb, pair, odd, lats, width)
            for r, (m, i), (c, ci) in zip(halo, msgs, cors):
                load_row(u, tabs[0][1][("u", 0, r)], m[i, 0:lats], c[ci], lats)
            where = Where()
            for ref, table in zip(before, earlier):
                where.add(ref, table)
            for ref, (_, table) in zip(outs, tabs):
                where.add(ref, table)
            faces(where, rows, fe_rows, width)

        return kernel

    kb_a, kb_b = tabs_a[1][1], tabs_b[1][1]
    fe_tab_a, fe_tab_b = tabs_a[5][1], tabs_b[5][1]
    set_b = call(
        setup_halo(tabs_b, (kb_a, fe_tab_a), halo_b, rows_b, fe_b, (FAR, 0)),
        (from_west, from_east, corner_west, corner_east, set_a[1], set_a[5]),
        shapes(tabs_b),
        [],
        "near",
    )
    set_c = call(
        setup_halo(tabs_c, (kb_b, fe_tab_b), halo_c, rows_c, fe_c, (0, NEAR)),
        (far_west, far_east, corner_west, corner_east, set_b[1], set_b[5]),
        shapes(tabs_c),
        [],
        "far",
    )

    done_b = [r for s, a, b in todo_b if s == STEPS for r in a + b]
    scratch = [pltpu.VMEM((2, 2, width, 128), F32)] * 2

    def flops(todo):
        return sum(len(a + b) for _, a, b in todo) * width * 1536 * 256 * 2

    def stage(todo, at, final):
        blocks = blocks_of(todo)

        def kernel(tables, n_in, *refs):
            ins, (wh_ref, wl_ref), rest = refs[:n_in], refs[n_in : n_in + 2], refs[n_in + 2 :]
            where = Where()
            for ref, table in zip(ins, tables):
                where.add(ref, table)
            levels, v, vl = rest[0], rest[-2], rest[-1]
            where.add(levels, at)

            def emit(s, r, x):
                if s == STEPS:
                    final(rest, r, x)
                else:
                    levels[pl.ds(at[("u", s, r)], width), :] = x

            def run(a0, a1, b0, b1):
                advance(where, blocks, width, wh_ref, wl_ref, v, vl, emit, ((a0, a1), (b0, b1)))

            pl.run_scoped(run, *[pltpu.ACC(q)((width, 256), F32) for q in (0, 0, 1, 1)])

        return kernel

    def used(tabs):
        return [i for i in range(len(tabs)) if i != 1]

    keys_a, keys_b, keys_c = later(todo_a, 99), later(todo_b, STEPS), later(todo_c, STEPS)
    at_a, at_b, at_c = (place(k, width) for k in (keys_a, keys_b, keys_c))

    ins_a = [set_a[i] for i in used(tabs_a)]
    tables_a = [tabs_a[i][1] for i in used(tabs_a)]
    kernel_a = stage(todo_a, at_a, None)
    (lev_a,) = call(
        lambda *refs: kernel_a(tables_a, len(ins_a), *refs),
        (*ins_a, wh, wl),
        [flat(len(keys_a))],
        scratch,
        "inner",
        flops(todo_a),
    )

    def final_b(rest, r, x):
        rest[1][done_b.index(r)] = x[PAD : PAD + lats]

    ins_b = ins_a + [lev_a] + [set_b[i] for i in used(tabs_b)]
    tables_b = tables_a + [at_a] + [tabs_b[i][1] for i in used(tabs_b)]
    kernel_b = stage(todo_b, at_b, final_b)
    lev_b, done = call(
        lambda *refs: kernel_b(tables_b, len(ins_b), *refs),
        (*ins_b, wh, wl),
        [flat(len(keys_b)), arr(len(done_b), lats, lev)],
        scratch,
        "middle",
        flops(todo_b),
    )

    def final_c(rest, r, x):
        rest[2][r] = x[PAD : PAD + lats]

    ins_c = ins_b + [lev_b] + [set_c[i] for i in used(tabs_c)]
    tables_c = tables_b + [at_b] + [tabs_c[i][1] for i in used(tabs_c)]
    kernel_c = stage(todo_c, at_c, final_c)

    def outer(*refs):
        n = len(ins_c) + 2
        done_ref, out, levels, v, vl = refs[n:]
        for i, r in enumerate(done_b):
            out[r] = done_ref[i]
        kernel_c(tables_c, len(ins_c), *refs[:n], levels, done_ref, out, v, vl)

    c_levels = flat(len(keys_c))
    (out,) = call(
        outer,
        (*ins_c, wh, wl, done),
        [arr(*field.shape)],
        [pltpu.VMEM(c_levels.shape, F32)] + scratch,
        "outer",
        flops(todo_c),
        16 << 20,
    )
    return out


def solution(mesh):
    return jax.shard_map(
        body,
        mesh=mesh,
        in_specs=(P("lon", "lat", None), P("lon", "lat"), P("lon", "lat"), P()),
        out_specs=P("lon", "lat", None),
        check_vma=False,
    )
```

```python
import jax
import jax.numpy as jnp
from jax import lax
from jax.experimental import pallas as pl
from jax.experimental.pallas import tpu as pltpu
from jax.sharding import PartitionSpec as P

STEPS = 6
NEAR = 3
FAR = STEPS - NEAR
PAD = 8
EDGE = 8
F32, BF16 = jnp.float32, jnp.bfloat16


def level_rows(near, before, lon):
    todo = []
    for s in range(1, STEPS + 1):
        low, high = s - near, lon - 1 + near - s
        if low > high:
            continue
        if before is not None and s - before <= lon - 1 + before - s:
            todo.append((s, list(range(low, s - before)), list(range(lon + before - s, high + 1))))
        else:
            todo.append((s, list(range(low, high + 1)), []))
    return todo


def blocks_of(todo):
    out = []
    for s, left, right in todo:
        rows = left + right
        out += [(s, rows[i], rows[i + 1]) for i in range(0, len(rows), 2)]
    return out


def place(keys, width):
    return {key: EDGE + i * width for i, key in enumerate(keys)}


class Where:
    def __init__(self):
        self.at = {}

    def add(self, ref, table):
        for key, base in table.items():
            self.at[key] = (ref, base)

    def __getitem__(self, key):
        return self.at[key]


def swaps(size):
    first = [(i, i + 1) for i in range(0, size, 2)]
    second = [(i + 1, (i + 2) % size) for i in range(0, size, 2)]
    return [pairs + [(j, i) for i, j in pairs] for pairs in (first, second)]


def is_even(axis):
    return lax.rem(lax.axis_index(axis), 2) == 0


def pick(even, a, b):
    return jnp.where(even, a, b)


def pack_kernel(lon, lats):
    def kernel(*refs):
        sources, (to_first, to_second, small, field, held), (k_ref, c_ref, sem) = refs[:4], refs[4:9], refs[9:]
        targets = (k_ref, c_ref, field, held)
        copies = [pltpu.make_async_copy(a, b, sem.at[i]) for i, (a, b) in enumerate(zip(sources, targets))]
        for copy in copies:
            copy.start()
        for copy in copies[:3]:
            copy.wait()
        even = is_even("lat")
        k, c = k_ref[...], c_ref[...].astype(F32)
        small[0:lon] = k
        small[lon : 2 * lon] = c
        lane = lax.broadcasted_iota(jnp.int32, (lon, 128), 1)
        sub = lax.broadcasted_iota(jnp.int32, (8, 128), 0)
        k_first, k_last = k[:, :128], k[:, lats - 128 :]
        c_first, c_last = c[:, :128], c[:, lats - 128 :]
        line_n = jnp.where(lane < 64, pltpu.roll(k_last, 8, 1), pltpu.roll(c_last, 72, 1))
        line_s = jnp.where(lane < 64, k_first, pltpu.roll(c_first, 64, 1))
        for r in range(lon):
            to_north = jnp.where(sub == 0, line_n[r : r + 1], field[r, lats - 8 : lats])
            to_south = jnp.where(sub == 7, line_s[r : r + 1], field[r, 0:8])
            to_first[r] = pick(even, to_north, to_south)
            to_second[r] = pick(even, to_south, to_north)
        copies[3].wait()

    return kernel


def message_kernel(lon, lats):
    def kernel(lat_first, lat_second, field, small, corners, near_1, near_2, far_1, far_2):
        even, even_lat = is_even("lon"), is_even("lat")
        lat, n_lat = lax.axis_index("lat"), lax.axis_size("lat")
        has_s = jnp.where(lat > 0, 1.0, 0.0).astype(F32)
        has_n = jnp.where(lat < n_lat - 1, 1.0, 0.0).astype(F32)
        for r in range(lon):
            corners[r, 0:8] = pick(even_lat, lat_second[r], lat_first[r]) * has_s
            corners[r, 8:16] = pick(even_lat, lat_first[r], lat_second[r]) * has_n
        k, c = small[0:lon], small[lon : 2 * lon]
        parts = [x[:, h * 128 : (h + 1) * 128] for x in (k, c) for h in range(lats // 128)]
        pad = jnp.zeros((8 - len(parts), 128), F32)
        metas = [jnp.concatenate([p[r : r + 1] for p in parts] + [pad]) for r in range(lon)]

        def rows(one, two, east, west):
            for i in range(one.shape[0]):
                e, w = east + i, west + i
                for j in range(0, lats, 32):
                    x, y = field[e, j : j + 32], field[w, j : j + 32]
                    one[i, j : j + 32] = pick(even, x, y)
                    two[i, j : j + 32] = pick(even, y, x)
                x, y = metas[e], metas[w]
                one[i, lats : lats + 8] = pick(even, x, y)
                two[i, lats : lats + 8] = pick(even, y, x)
                x, y = corners[e], corners[w]
                one[i, lats + 8 : lats + 24] = pick(even, x, y)
                two[i, lats + 8 : lats + 24] = pick(even, y, x)

        rows(near_1, near_2, lon - NEAR, 0)
        rows(far_1, far_2, lon - STEPS, NEAR)

    return kernel


def split3(x):
    high = x.astype(BF16).astype(F32)
    mid = (x - high).astype(BF16).astype(F32)
    return [high, mid, x - high - mid]


def spread(lines, kinds, sides, rows_at, kb, pair, odd, lats, width):
    k = lax.broadcasted_iota(jnp.int32, (32, 256), 0)
    lane = lax.broadcasted_iota(jnp.int32, (32, 256), 1)
    dims = (((0,), (0,)), ((), ()))

    def put(at, n, value):
        half = jnp.floor(value * 0.5)
        pair[pl.ds(at, n), :] = half
        odd[pl.ds(at, n), :] = value - 2.0 * half

    mine = lax.rem(k, 8)
    full = [jnp.concatenate(split3(a) + [c]).astype(BF16) for a, c in zip(lines, kinds)]
    edge = [jnp.concatenate(split3(a) + [jnp.zeros((8, 128), F32)]).astype(BF16) for a in sides]
    for i, at in enumerate(rows_at):
        hit = (mine == i) & ((k >= 24) == (lane >= 128))
        one = jnp.where(hit, 1.0, 0.0).astype(BF16)
        for h, x in enumerate(full):
            got = lax.dot_general(x, one, dims, preferred_element_type=F32)
            here = at + PAD + h * 128
            kb[pl.ds(here, 128), :] = got[:, :128]
            put(here, 128, got[:, 128:])
        for x, here in zip(edge, (at, at + PAD + lats)):
            got = lax.dot_general(x, one, dims, preferred_element_type=F32)
            kb[pl.ds(here, 8), :] = got[0:8, :128]
            put(here, 8, got[64:72, :128])


def load_row(ref, base, middle, sides, lats):
    sub = lax.broadcasted_iota(jnp.int32, (8, 128), 0)
    ref[pl.ds(base, 8), :] = jnp.where(sub == 0, 0.0, sides[0:8])
    for j in range(0, lats, 32):
        ref[pl.ds(base + PAD + j, 32), :] = middle(j, j + 32)
    ref[pl.ds(base + PAD + lats, 8), :] = jnp.where(sub == 7, 0.0, sides[8:16])


def faces(where, rows, fe_rows, width):
    for r in fe_rows:
        a, ab = where[("kb", 0, r)]
        b, bb = where[("kb", 0, r + 1)]
        o, ob = where[("fe", 0, r)]
        for j in range(0, width, 8):
            o[pl.ds(ob + j, 8), :] = 0.5 * (a[pl.ds(ab + j, 8), :] + b[pl.ds(bb + j, 8), :])
    for r in rows:
        k, kb = where[("kb", 0, r)]
        e, eb = where[("fe", 0, r)]
        w, wb = where[("fe", 0, r - 1)]
        z, zb = where[("c0", 0, r)]
        n, nb = where[("fn", 0, r)]
        for j in range(0, width, 8):
            mid = k[pl.ds(kb + j, 8), :]
            up = k[pl.ds(kb + j + 1, 8), :]
            fn = 0.5 * (mid + up)
            fs = 0.5 * (mid + k[pl.ds(kb + j - 1, 8), :])
            c0 = 1.0 - e[pl.ds(eb + j, 8), :] - w[pl.ds(wb + j, 8), :] - fn - fs
            z[pl.ds(zb + j, 8), :] = jnp.where(mid > 0.0, c0, 0.0)
            n[pl.ds(nb + j, 8), :] = jnp.where((mid > 0.0) & (up > 0.0), fn, 0.0)


def advance(where, blocks, width, wh, wl, v, vl, emit, accs):
    def explicit(b):
        s, *rows = blocks[b]
        for q, r in enumerate(rows):
            cref, cb = where[("u", s - 1, r)]
            wref, wb = where[("u", s - 1, r - 1)]
            eref, eb = where[("u", s - 1, r + 1)]
            zref, zb = where[("c0", 0, r)]
            gref, gb = where[("fe", 0, r)]
            href, hb = where[("fe", 0, r - 1)]
            nref, nb = where[("fn", 0, r)]
            for j in range(0, width, 8):
                d = lambda base: pl.ds(base + j, 8)
                x = zref[d(zb), :] * cref[d(cb), :]
                x = x + gref[d(gb), :] * eref[d(eb), :]
                x = x + href[d(hb), :] * wref[d(wb), :]
                x = x + nref[d(nb), :] * cref[d(cb + 1), :]
                x = x + nref[d(nb - 1), :] * cref[d(cb - 1), :]
                v[b % 2, q, j : j + 8] = x
                vl[b % 2, q, j : j + 8] = x - x.astype(BF16).astype(F32)

    tiles = [(x, w, t) for t in range(2) for x, w in ((v, wh), (v, wl), (vl, wh))]

    def push(k):
        _, w, t = tiles[k]
        for q in range(2):
            pltpu.matmul_push_rhs(w[t * 256 : (t + 1) * 256, :], staging_register=k % 2, mxu_index=q)

    def products(b):
        _, *rows = blocks[b]
        push(0)
        for k, (x, _, t) in enumerate(tiles):
            if k + 1 < len(tiles):
                push(k + 1)
            for q, r in enumerate(rows):
                pref, pb = where[("pair", 0, r)]
                pair = pref[pl.ds(pb, width), :]
                value = x[b % 2, q]
                lhs = [jnp.where(pair == float(2 * t + i), value, 0.0) for i in range(2)]
                pltpu.matmul_acc_lhs(accs[q][b % 2], jnp.concatenate(lhs, axis=1), load_staged_rhs=k % 2)

    def finish(b):
        s, *rows = blocks[b]
        for q, r in enumerate(rows):
            got = pltpu.matmul_pop(accs[q][b % 2])
            oref, ob = where[("odd", 0, r)]
            odd = oref[pl.ds(ob, width), :]
            emit(s, r, jnp.where(odd > 0.5, got[:, 128:], got[:, :128]))

    for b, (s, *rows) in enumerate(blocks):
        need = {r + d for r in rows for d in (-1, 0, 1)}
        wait = b > 0 and blocks[b - 1][0] == s - 1 and bool(need & set(blocks[b - 1][1:]))
        if wait:
            finish(b - 1)
        explicit(b)
        products(b)
        if b > 0 and not wait:
            finish(b - 1)
    finish(len(blocks) - 1)


def call(kernel, ins, outs, scratch, name, flops=0, limit=8 << 20):
    vmem = pl.BlockSpec(memory_space=pltpu.VMEM)
    return pl.pallas_call(
        kernel,
        out_shape=outs,
        in_specs=[vmem] * len(ins),
        out_specs=[vmem] * len(outs),
        scratch_shapes=scratch,
        compiler_params=pltpu.CompilerParams(vmem_limit_bytes=limit),
        cost_estimate=pl.CostEstimate(flops=flops, bytes_accessed=1 << 20, transcendentals=0),
        name=name,
    )(*ins)


def body(field, kappa, classes, inverses):
    lon, lats, lev = field.shape
    width = lats + 2 * PAD
    n_lon, n_lat = lax.axis_size("lon"), lax.axis_size("lat")
    lon_swaps, lat_swaps = swaps(n_lon), swaps(n_lat)
    halves = lats // 128

    def arr(*shape, dtype=F32):
        return jax.ShapeDtypeStruct(shape, dtype)

    def flat(n):
        return arr(n * width + 2 * EDGE, 128)

    edge, near, far = (lon, 8, 128), (NEAR, lats + 24, 128), (FAR, lats + 24, 128)
    hbm, vmem = pl.BlockSpec(memory_space=pltpu.HBM), pl.BlockSpec(memory_space=pltpu.VMEM)
    inputs = [pltpu.with_memory_space_constraint(x, pltpu.HBM) for x in (kappa, classes, field, inverses)]
    *to_lat, small, field, inverses = pl.pallas_call(
        pack_kernel(lon, lats),
        out_shape=[arr(*edge), arr(*edge), arr(2 * lon, lats), arr(*field.shape), arr(*inverses.shape)],
        in_specs=[hbm] * 4,
        out_specs=[vmem] * 5,
        scratch_shapes=[
            pltpu.VMEM(kappa.shape, F32),
            pltpu.VMEM(classes.shape, jnp.int32),
            pltpu.SemaphoreType.DMA((4,)),
        ],
        compiler_params=pltpu.CompilerParams(vmem_limit_bytes=8 << 20),
        name="pack",
    )(*inputs)
    from_lat = [lax.ppermute(x, "lat", pairs) for x, pairs in zip(to_lat, lat_swaps)]
    corners, *to_lon = call(
        message_kernel(lon, lats),
        (*from_lat, field, small),
        [arr(lon, 16, 128), arr(*near), arr(*near), arr(*far), arr(*far)],
        [],
        "message",
    )
    near_1, near_2, far_1, far_2 = [lax.ppermute(x, "lon", pairs) for x, pairs in zip(to_lon, lon_swaps * 2)]

    todo_a, todo_b, todo_c = level_rows(0, None, lon), level_rows(NEAR, 0, lon), level_rows(STEPS, NEAR, lon)

    def later(todo, last):
        return [("u", s, r) for s, a, b in todo for r in a + b if s < last]

    own = list(range(lon))
    halo_b = list(range(-NEAR, 0)) + list(range(lon, lon + NEAR))
    halo_c = list(range(-STEPS, -NEAR)) + list(range(lon + NEAR, lon + STEPS))
    rows_a, fe_a = own[1:-1], own[:-1]
    rows_b = list(range(1 - NEAR, 1)) + list(range(lon - 1, lon - 1 + NEAR))
    fe_b = list(range(-NEAR, 0)) + list(range(lon - 1, lon - 1 + NEAR))
    rows_c = list(range(1 - STEPS, 1 - NEAR)) + list(range(lon - 1 + NEAR, lon - 1 + STEPS))
    fe_c = list(range(-STEPS, -NEAR)) + list(range(lon - 1 + NEAR, lon - 1 + STEPS))

    def at0(name, rows):
        return place([(name, 0, r) for r in rows], width)

    def phase_tables(halo, rows, fe_rows):
        names = [("u", halo), ("kb", halo), ("pair", halo), ("odd", halo), ("c0", rows), ("fe", fe_rows), ("fn", rows)]
        return [(len(rs), at0(name, rs)) for name, rs in names]

    tabs_a = phase_tables(own, rows_a, fe_a)
    tabs_b = phase_tables(halo_b, rows_b, fe_b)
    tabs_c = phase_tables(halo_c, rows_c, fe_c)

    def shapes(tabs):
        return [flat(n) for n, _ in tabs]

    def found(*pairs):
        where = Where()
        for refs, tabs in pairs:
            for ref, (_, table) in zip(refs, tabs):
                where.add(ref, table)
        return where

    def stack8(rows):
        return jnp.concatenate(rows + [jnp.zeros((8 - len(rows), 128), F32)] * (len(rows) < 8))

    def msg_lines(rows, which):
        at = [lats + which * halves + h for h in range(halves)]
        return [stack8([row(x, x + 1) for row in rows]) for x in at]

    def side_lines(rows):
        return [stack8([row(at, at + 1) for row in rows]) for at in (0, 15)]

    def weights_kernel(inv_ref, wh, wl):
        for kind in range(inv_ref.shape[0]):
            w = inv_ref[kind].T
            high = w.astype(BF16)
            here = (slice((kind // 2) * lev, (kind // 2 + 1) * lev), slice((kind % 2) * lev, (kind % 2 + 1) * lev))
            wh[here] = high
            wl[here] = (w - high.astype(F32)).astype(BF16)

    def setup_a(field_ref, small_ref, corners_ref, u, kb, pair, odd, c0, fe, fn):
        k, c = small_ref[0:lon], small_ref[lon : 2 * lon]
        lines = [k[:, h * 128 : (h + 1) * 128] for h in range(halves)]
        kinds = [c[:, h * 128 : (h + 1) * 128] for h in range(halves)]
        at = tabs_a[1][1]
        sides = side_lines([lambda a, b, r=r: corners_ref[r, a:b] for r in own])
        spread(lines, kinds, sides, [at[("kb", 0, r)] for r in own], kb, pair, odd, lats, width)
        for r in own:
            load_row(u, tabs_a[0][1][("u", 0, r)], lambda a, b, r=r: field_ref[r, a:b], corners_ref[r], lats)
        faces(found(((u, kb, pair, odd, c0, fe, fn), tabs_a)), rows_a, fe_a, width)

    pairs_n = inverses.shape[0] // 2
    weights = arr(pairs_n * lev, 2 * lev, dtype=BF16)
    wh, wl = call(weights_kernel, (inverses,), [weights] * 2, [], "weights")
    set_a = call(setup_a, (field, small, corners), shapes(tabs_a), [], "own")

    def setup_halo(tabs, earlier, halo, rows, fe_rows):
        half = len(halo) // 2

        def kernel(*refs):
            even = is_even("lon")
            one, two, *rest = refs
            before, outs = rest[: len(earlier)], rest[len(earlier) :]
            u, kb, pair, odd, c0, fe, fn = outs
            sources = [(two, one, i) for i in range(half)] + [(one, two, i) for i in range(half)]
            msgs = [lambda a, b, s=s: pick(even, s[0][s[2], a:b], s[1][s[2], a:b]) for s in sources]
            cors = [lambda a, b, m=m: m(lats + 8 + a, lats + 8 + b) for m in msgs]
            at = [tabs[1][1][("kb", 0, r)] for r in halo]
            spread(msg_lines(msgs, 0), msg_lines(msgs, 1), side_lines(cors), at, kb, pair, odd, lats, width)
            for r, m, c in zip(halo, msgs, cors):
                load_row(u, tabs[0][1][("u", 0, r)], m, c(0, 16), lats)
            where = Where()
            for ref, table in zip(before, earlier):
                where.add(ref, table)
            for ref, (_, table) in zip(outs, tabs):
                where.add(ref, table)
            faces(where, rows, fe_rows, width)

        return kernel

    kb_a, kb_b = tabs_a[1][1], tabs_b[1][1]
    fe_tab_a, fe_tab_b = tabs_a[5][1], tabs_b[5][1]
    set_b = call(
        setup_halo(tabs_b, (kb_a, fe_tab_a), halo_b, rows_b, fe_b),
        (near_1, near_2, set_a[1], set_a[5]),
        shapes(tabs_b),
        [],
        "near",
    )
    set_c = call(
        setup_halo(tabs_c, (kb_b, fe_tab_b), halo_c, rows_c, fe_c),
        (far_1, far_2, set_b[1], set_b[5]),
        shapes(tabs_c),
        [],
        "far",
    )

    done_b = [r for s, a, b in todo_b if s == STEPS for r in a + b]
    scratch = [pltpu.VMEM((2, 2, width, 128), F32)] * 2

    def flops(todo):
        return sum(len(a + b) for _, a, b in todo) * width * 1536 * 256 * 2

    def stage(todo, at, final):
        blocks = blocks_of(todo)

        def kernel(tables, n_in, *refs):
            ins, (wh_ref, wl_ref), rest = refs[:n_in], refs[n_in : n_in + 2], refs[n_in + 2 :]
            where = Where()
            for ref, table in zip(ins, tables):
                where.add(ref, table)
            levels, v, vl = rest[0], rest[-2], rest[-1]
            where.add(levels, at)

            def emit(s, r, x):
                if s == STEPS:
                    final(rest, r, x)
                else:
                    levels[pl.ds(at[("u", s, r)], width), :] = x

            def run(a0, a1, b0, b1):
                advance(where, blocks, width, wh_ref, wl_ref, v, vl, emit, ((a0, a1), (b0, b1)))

            pl.run_scoped(run, *[pltpu.ACC(q)((width, 256), F32) for q in (0, 0, 1, 1)])

        return kernel

    def used(tabs):
        return [i for i in range(len(tabs)) if i != 1]

    keys_a, keys_b, keys_c = later(todo_a, 99), later(todo_b, STEPS), later(todo_c, STEPS)
    at_a, at_b, at_c = (place(k, width) for k in (keys_a, keys_b, keys_c))

    ins_a = [set_a[i] for i in used(tabs_a)]
    tables_a = [tabs_a[i][1] for i in used(tabs_a)]
    kernel_a = stage(todo_a, at_a, None)
    (lev_a,) = call(
        lambda *refs: kernel_a(tables_a, len(ins_a), *refs),
        (*ins_a, wh, wl),
        [flat(len(keys_a))],
        scratch,
        "inner",
        flops(todo_a),
    )

    def final_b(rest, r, x):
        rest[1][done_b.index(r)] = x[PAD : PAD + lats]

    ins_b = ins_a + [lev_a] + [set_b[i] for i in used(tabs_b)]
    tables_b = tables_a + [at_a] + [tabs_b[i][1] for i in used(tabs_b)]
    kernel_b = stage(todo_b, at_b, final_b)
    lev_b, done = call(
        lambda *refs: kernel_b(tables_b, len(ins_b), *refs),
        (*ins_b, wh, wl),
        [flat(len(keys_b)), arr(len(done_b), lats, lev)],
        scratch,
        "middle",
        flops(todo_b),
    )

    def final_c(rest, r, x):
        rest[2][r] = x[PAD : PAD + lats]

    ins_c = ins_b + [lev_b] + [set_c[i] for i in used(tabs_c)]
    tables_c = tables_b + [at_b] + [tabs_c[i][1] for i in used(tabs_c)]
    kernel_c = stage(todo_c, at_c, final_c)

    def outer(*refs):
        n = len(ins_c) + 2
        done_ref, out, levels, v, vl = refs[n:]
        for i, r in enumerate(done_b):
            out[r] = done_ref[i]
        kernel_c(tables_c, len(ins_c), *refs[:n], levels, done_ref, out, v, vl)

    c_levels = flat(len(keys_c))
    (out,) = call(
        outer,
        (*ins_c, wh, wl, done),
        [arr(*field.shape)],
        [pltpu.VMEM(c_levels.shape, F32)] + scratch,
        "outer",
        flops(todo_c),
        16 << 20,
    )
    return out


def solution(mesh):
    return jax.shard_map(
        body,
        mesh=mesh,
        in_specs=(P("lon", "lat", None), P("lon", "lat"), P("lon", "lat"), P()),
        out_specs=P("lon", "lat", None),
        check_vma=False,
    )
```

```python
import jax
import jax.numpy as jnp
from jax import lax
from jax.experimental import pallas as pl
from jax.experimental.pallas import tpu as pltpu
from jax.sharding import PartitionSpec as P

STEPS = 6
NEAR = 3
FAR = STEPS - NEAR
PAD = 8
EDGE = 8
GAP = 0
PIECE = 48
F32, BF16 = jnp.float32, jnp.bfloat16


def level_rows(near, before, lon):
    todo = []
    for s in range(1, STEPS + 1):
        low, high = s - near, lon - 1 + near - s
        if low > high:
            continue
        if before is not None and s - before <= lon - 1 + before - s:
            todo.append((s, list(range(low, s - before)), list(range(lon + before - s, high + 1))))
        else:
            todo.append((s, list(range(low, high + 1)), []))
    return todo


def blocks_of(todo):
    out = []
    for s, left, right in todo:
        rows = left + right
        out += [(s, rows[i], rows[i + 1]) for i in range(0, len(rows), 2)]
    return out


def place(keys, width):
    return {key: EDGE + i * (width + GAP) for i, key in enumerate(keys)}


class Where:
    def __init__(self):
        self.at = {}

    def add(self, ref, table):
        for key, base in table.items():
            self.at[key] = (ref, base)

    def __getitem__(self, key):
        return self.at[key]


def swaps(size):
    first = [(i, i + 1) for i in range(0, size, 2)]
    second = [(i + 1, (i + 2) % size) for i in range(0, size, 2)]
    return [pairs + [(j, i) for i, j in pairs] for pairs in (first, second)]


def is_even(axis):
    return lax.rem(lax.axis_index(axis), 2) == 0


def pick(even, a, b):
    return jnp.where(even, a, b)


def pack_kernel(lon, lats):
    def kernel(*refs):
        sources, (to_first, to_second, small, field, held), (k_ref, c_ref, sem) = refs[:4], refs[4:9], refs[9:]
        targets = (k_ref, c_ref, field, held)
        copies = [pltpu.make_async_copy(a, b, sem.at[i]) for i, (a, b) in enumerate(zip(sources, targets))]
        for copy in copies:
            copy.start()
        for copy in copies[:3]:
            copy.wait()
        even = is_even("lat")
        k, c = k_ref[...], c_ref[...].astype(F32)
        small[0:lon] = k
        small[lon : 2 * lon] = c
        lane = lax.broadcasted_iota(jnp.int32, (lon, 128), 1)
        sub = lax.broadcasted_iota(jnp.int32, (8, 128), 0)
        k_first, k_last = k[:, :128], k[:, lats - 128 :]
        c_first, c_last = c[:, :128], c[:, lats - 128 :]
        line_n = jnp.where(lane < 64, pltpu.roll(k_last, 8, 1), pltpu.roll(c_last, 72, 1))
        line_s = jnp.where(lane < 64, k_first, pltpu.roll(c_first, 64, 1))
        for r in range(lon):
            to_north = jnp.where(sub == 0, line_n[r : r + 1], field[r, lats - 8 : lats])
            to_south = jnp.where(sub == 7, line_s[r : r + 1], field[r, 0:8])
            to_first[r] = pick(even, to_north, to_south)
            to_second[r] = pick(even, to_south, to_north)
        copies[3].wait()

    return kernel


def message_kernel(lon, lats):
    def kernel(lat_first, lat_second, field, small, corners, near_1, near_2, far_1, far_2):
        even, even_lat = is_even("lon"), is_even("lat")
        lat, n_lat = lax.axis_index("lat"), lax.axis_size("lat")
        has_s = jnp.where(lat > 0, 1.0, 0.0).astype(F32)
        has_n = jnp.where(lat < n_lat - 1, 1.0, 0.0).astype(F32)
        for r in range(lon):
            corners[r, 0:8] = pick(even_lat, lat_second[r], lat_first[r]) * has_s
            corners[r, 8:16] = pick(even_lat, lat_first[r], lat_second[r]) * has_n
        k, c = small[0:lon], small[lon : 2 * lon]
        parts = [x[:, h * 128 : (h + 1) * 128] for x in (k, c) for h in range(lats // 128)]
        pad = jnp.zeros((8 - len(parts), 128), F32)
        metas = [jnp.concatenate([p[r : r + 1] for p in parts] + [pad]) for r in range(lon)]

        def rows(one, two, east, west):
            for i in range(one.shape[0]):
                e, w = east + i, west + i
                for j in range(0, lats, 32):
                    x, y = field[e, j : j + 32], field[w, j : j + 32]
                    one[i, j : j + 32] = pick(even, x, y)
                    two[i, j : j + 32] = pick(even, y, x)
                x, y = metas[e], metas[w]
                one[i, lats : lats + 8] = pick(even, x, y)
                two[i, lats : lats + 8] = pick(even, y, x)
                x, y = corners[e], corners[w]
                one[i, lats + 8 : lats + 24] = pick(even, x, y)
                two[i, lats + 8 : lats + 24] = pick(even, y, x)

        rows(near_1, near_2, lon - NEAR, 0)
        rows(far_1, far_2, lon - STEPS, NEAR)

    return kernel


def split3(x):
    high = x.astype(BF16).astype(F32)
    mid = (x - high).astype(BF16).astype(F32)
    return [high, mid, x - high - mid]


def spread(lines, kinds, sides, rows_at, kb, pair, odd, lats, width):
    k = lax.broadcasted_iota(jnp.int32, (32, 256), 0)
    lane = lax.broadcasted_iota(jnp.int32, (32, 256), 1)
    dims = (((0,), (0,)), ((), ()))

    def put(at, n, value):
        half = jnp.floor(value * 0.5)
        pair[pl.ds(at, n), :] = half
        odd[pl.ds(at, n), :] = value - 2.0 * half

    mine = lax.rem(k, 8)
    full = [jnp.concatenate(split3(a) + [c]).astype(BF16) for a, c in zip(lines, kinds)]
    edge = [jnp.concatenate(split3(a) + [jnp.zeros((8, 128), F32)]).astype(BF16) for a in sides]
    for i, at in enumerate(rows_at):
        hit = (mine == i) & ((k >= 24) == (lane >= 128))
        one = jnp.where(hit, 1.0, 0.0).astype(BF16)
        for h, x in enumerate(full):
            got = lax.dot_general(x, one, dims, preferred_element_type=F32)
            here = at + PAD + h * 128
            kb[pl.ds(here, 128), :] = got[:, :128]
            put(here, 128, got[:, 128:])
        for x, here in zip(edge, (at, at + PAD + lats)):
            got = lax.dot_general(x, one, dims, preferred_element_type=F32)
            kb[pl.ds(here, 8), :] = got[0:8, :128]
            put(here, 8, got[64:72, :128])


def load_row(ref, base, middle, sides, lats):
    sub = lax.broadcasted_iota(jnp.int32, (8, 128), 0)
    ref[pl.ds(base, 8), :] = jnp.where(sub == 0, 0.0, sides[0:8])
    for j in range(0, lats, 32):
        ref[pl.ds(base + PAD + j, 32), :] = middle(j, j + 32)
    ref[pl.ds(base + PAD + lats, 8), :] = jnp.where(sub == 7, 0.0, sides[8:16])


def faces(where, rows, fe_rows, width):
    for r in fe_rows:
        a, ab = where[("kb", 0, r)]
        b, bb = where[("kb", 0, r + 1)]
        o, ob = where[("fe", 0, r)]
        for j in range(0, width, 8):
            o[pl.ds(ob + j, 8), :] = 0.5 * (a[pl.ds(ab + j, 8), :] + b[pl.ds(bb + j, 8), :])
    for r in rows:
        k, kb = where[("kb", 0, r)]
        e, eb = where[("fe", 0, r)]
        w, wb = where[("fe", 0, r - 1)]
        z, zb = where[("c0", 0, r)]
        n, nb = where[("fn", 0, r)]
        for j in range(0, width, 8):
            mid = k[pl.ds(kb + j, 8), :]
            up = k[pl.ds(kb + j + 1, 8), :]
            fn = 0.5 * (mid + up)
            fs = 0.5 * (mid + k[pl.ds(kb + j - 1, 8), :])
            c0 = 1.0 - e[pl.ds(eb + j, 8), :] - w[pl.ds(wb + j, 8), :] - fn - fs
            z[pl.ds(zb + j, 8), :] = jnp.where(mid > 0.0, c0, 0.0)
            n[pl.ds(nb + j, 8), :] = jnp.where((mid > 0.0) & (up > 0.0), fn, 0.0)


def pieces(width):
    return [(j, min(PIECE, width - j)) for j in range(0, width, PIECE)]


def advance(where, blocks, width, wh, wl, v, vl, emit, accs):
    tiles = [(x, w, t) for t in range(2) for x, w in ((v, wh), (v, wl), (vl, wh))]
    quarter = len(tiles) - 2

    def explicit(b, parts):
        s, *rows = blocks[b]
        todo = [(q, r, j) for j in range(0, width, 8) for q, r in enumerate(rows)]
        for q, r, j in [x for i, x in enumerate(todo) if i * quarter // len(todo) in parts]:
            cref, cb = where[("u", s - 1, r)]
            wref, wb = where[("u", s - 1, r - 1)]
            eref, eb = where[("u", s - 1, r + 1)]
            zref, zb = where[("c0", 0, r)]
            gref, gb = where[("fe", 0, r)]
            href, hb = where[("fe", 0, r - 1)]
            nref, nb = where[("fn", 0, r)]
            d = lambda base: pl.ds(base + j, 8)
            x = zref[d(zb), :] * cref[d(cb), :]
            x = x + gref[d(gb), :] * eref[d(eb), :]
            x = x + href[d(hb), :] * wref[d(wb), :]
            x = x + nref[d(nb), :] * cref[d(cb + 1), :]
            x = x + nref[d(nb - 1), :] * cref[d(cb - 1), :]
            v[b % 2, q, j : j + 8] = x
            vl[b % 2, q, j : j + 8] = x - x.astype(BF16).astype(F32)

    def push(k):
        _, w, t = tiles[k]
        for q in range(2):
            tile = jnp.concatenate([w[h, t * 256 : (t + 1) * 256, :] for h in range(2)], axis=1)
            pltpu.matmul_push_rhs(tile, staging_register=k % 2, mxu_index=q)

    def product(b, k):
        x, _, t = tiles[k]
        for i, (j, m) in enumerate(pieces(width)):
            for q, r in enumerate(blocks[b][1:]):
                pref, pb = where[("pair", 0, r)]
                pair = pref[pl.ds(pb + j, m), :]
                value = x[b % 2, q, j : j + m]
                lhs = jnp.concatenate([jnp.where(pair == float(2 * t + h), value, 0.0) for h in range(2)], axis=1)
                pltpu.matmul_acc_lhs(accs[q][b % 2][i], lhs, load_staged_rhs=k % 2 if i == 0 else None)

    def finish(b):
        s, *rows = blocks[b]
        for i, (j, m) in enumerate(pieces(width)):
            for q, r in enumerate(rows):
                got = pltpu.matmul_pop(accs[q][b % 2][i])
                oref, ob = where[("odd", 0, r)]
                odd = oref[pl.ds(ob + j, m), :]
                emit(s, r, j, jnp.where(odd > 0.5, got[:, 128:], got[:, :128]))

    def depends(b):
        if b == 0 or b == len(blocks):
            return True
        need = {r + d for r in blocks[b][1:] for d in (-1, 0, 1)}
        return blocks[b - 1][0] == blocks[b][0] - 1 and bool(need & set(blocks[b - 1][1:]))

    every = range(quarter)
    for b in range(len(blocks)):
        if depends(b):
            explicit(b, every)
        push(0)
        for k in range(len(tiles)):
            if k + 1 < len(tiles):
                push(k + 1)
            product(b, k)
            if k == 1 and not depends(b):
                finish(b - 1)
            if k >= 2 and not depends(b + 1):
                explicit(b + 1, (k - 2,))
        if depends(b + 1):
            finish(b)


def call(kernel, ins, outs, scratch, name, flops=0, limit=8 << 20):
    vmem = pl.BlockSpec(memory_space=pltpu.VMEM)
    return pl.pallas_call(
        kernel,
        out_shape=outs,
        in_specs=[vmem] * len(ins),
        out_specs=[vmem] * len(outs),
        scratch_shapes=scratch,
        compiler_params=pltpu.CompilerParams(vmem_limit_bytes=limit),
        cost_estimate=pl.CostEstimate(flops=flops, bytes_accessed=1 << 20, transcendentals=0),
        name=name,
    )(*ins)


def body(field, kappa, classes, inverses):
    lon, lats, lev = field.shape
    width = lats + 2 * PAD
    n_lon, n_lat = lax.axis_size("lon"), lax.axis_size("lat")
    lon_swaps, lat_swaps = swaps(n_lon), swaps(n_lat)
    halves = lats // 128

    def arr(*shape, dtype=F32):
        return jax.ShapeDtypeStruct(shape, dtype)

    def flat(n):
        return arr(n * (width + GAP) + 2 * EDGE, 128)

    edge, near, far = (lon, 8, 128), (NEAR, lats + 24, 128), (FAR, lats + 24, 128)
    hbm, vmem = pl.BlockSpec(memory_space=pltpu.HBM), pl.BlockSpec(memory_space=pltpu.VMEM)
    inputs = [pltpu.with_memory_space_constraint(x, pltpu.HBM) for x in (kappa, classes, field, inverses)]
    *to_lat, small, field, inverses = pl.pallas_call(
        pack_kernel(lon, lats),
        out_shape=[arr(*edge), arr(*edge), arr(2 * lon, lats), arr(*field.shape), arr(*inverses.shape)],
        in_specs=[hbm] * 4,
        out_specs=[vmem] * 5,
        scratch_shapes=[
            pltpu.VMEM(kappa.shape, F32),
            pltpu.VMEM(classes.shape, jnp.int32),
            pltpu.SemaphoreType.DMA((4,)),
        ],
        compiler_params=pltpu.CompilerParams(vmem_limit_bytes=8 << 20),
        name="pack",
    )(*inputs)
    from_lat = [lax.ppermute(x, "lat", pairs) for x, pairs in zip(to_lat, lat_swaps)]
    corners, *to_lon = call(
        message_kernel(lon, lats),
        (*from_lat, field, small),
        [arr(lon, 16, 128), arr(*near), arr(*near), arr(*far), arr(*far)],
        [],
        "message",
    )
    near_1, near_2, far_1, far_2 = [lax.ppermute(x, "lon", pairs) for x, pairs in zip(to_lon, lon_swaps * 2)]

    todo_a, todo_b, todo_c = level_rows(0, None, lon), level_rows(NEAR, 0, lon), level_rows(STEPS, NEAR, lon)

    def later(todo, last):
        return [("u", s, r) for s, a, b in todo for r in a + b if s < last]

    own = list(range(lon))
    halo_b = list(range(-NEAR, 0)) + list(range(lon, lon + NEAR))
    halo_c = list(range(-STEPS, -NEAR)) + list(range(lon + NEAR, lon + STEPS))
    rows_a, fe_a = own[1:-1], own[:-1]
    rows_b = list(range(1 - NEAR, 1)) + list(range(lon - 1, lon - 1 + NEAR))
    fe_b = list(range(-NEAR, 0)) + list(range(lon - 1, lon - 1 + NEAR))
    rows_c = list(range(1 - STEPS, 1 - NEAR)) + list(range(lon - 1 + NEAR, lon - 1 + STEPS))
    fe_c = list(range(-STEPS, -NEAR)) + list(range(lon - 1 + NEAR, lon - 1 + STEPS))

    def at0(name, rows):
        return place([(name, 0, r) for r in rows], width)

    def phase_tables(halo, rows, fe_rows):
        names = [("u", halo), ("kb", halo), ("pair", halo), ("odd", halo), ("c0", rows), ("fe", fe_rows), ("fn", rows)]
        return [(len(rs), at0(name, rs)) for name, rs in names]

    tabs_a = phase_tables(own, rows_a, fe_a)
    tabs_b = phase_tables(halo_b, rows_b, fe_b)
    tabs_c = phase_tables(halo_c, rows_c, fe_c)

    def shapes(tabs):
        return [flat(n) for n, _ in tabs]

    def found(*pairs):
        where = Where()
        for refs, tabs in pairs:
            for ref, (_, table) in zip(refs, tabs):
                where.add(ref, table)
        return where

    def stack8(rows):
        return jnp.concatenate(rows + [jnp.zeros((8 - len(rows), 128), F32)] * (len(rows) < 8))

    def msg_lines(rows, which):
        at = [lats + which * halves + h for h in range(halves)]
        return [stack8([row(x, x + 1) for row in rows]) for x in at]

    def side_lines(rows):
        return [stack8([row(at, at + 1) for row in rows]) for at in (0, 15)]

    def weights_kernel(inv_ref, wh, wl):
        for kind in range(inv_ref.shape[0]):
            w = inv_ref[kind].T
            high = w.astype(BF16)
            here = (kind % 2, slice((kind // 2) * lev, (kind // 2 + 1) * lev))
            wh[here] = high
            wl[here] = (w - high.astype(F32)).astype(BF16)

    def setup_a(field_ref, small_ref, corners_ref, u, kb, pair, odd, c0, fe, fn):
        k, c = small_ref[0:lon], small_ref[lon : 2 * lon]
        lines = [k[:, h * 128 : (h + 1) * 128] for h in range(halves)]
        kinds = [c[:, h * 128 : (h + 1) * 128] for h in range(halves)]
        at = tabs_a[1][1]
        sides = side_lines([lambda a, b, r=r: corners_ref[r, a:b] for r in own])
        spread(lines, kinds, sides, [at[("kb", 0, r)] for r in own], kb, pair, odd, lats, width)
        for r in own:
            load_row(u, tabs_a[0][1][("u", 0, r)], lambda a, b, r=r: field_ref[r, a:b], corners_ref[r], lats)
        faces(found(((u, kb, pair, odd, c0, fe, fn), tabs_a)), rows_a, fe_a, width)

    pairs_n = inverses.shape[0] // 2
    weights = arr(2, pairs_n * lev, lev, dtype=BF16)
    wh, wl = call(weights_kernel, (inverses,), [weights] * 2, [], "weights")
    set_a = call(setup_a, (field, small, corners), shapes(tabs_a), [], "own")

    def setup_halo(tabs, earlier, halo, rows, fe_rows, last=False):
        half = len(halo) // 2

        def kernel(*refs):
            even = is_even("lon")
            one, two, *rest = refs
            before, outs = rest[: len(earlier)], rest[len(earlier) :]
            if last:
                outs = [outs[0], outs[-1], *outs[1:-1]]
            u, kb, pair, odd, c0, fe, fn = outs
            sources = [(two, one, i) for i in range(half)] + [(one, two, i) for i in range(half)]
            msgs = [lambda a, b, s=s: pick(even, s[0][s[2], a:b], s[1][s[2], a:b]) for s in sources]
            cors = [lambda a, b, m=m: m(lats + 8 + a, lats + 8 + b) for m in msgs]
            at = [tabs[1][1][("kb", 0, r)] for r in halo]
            spread(msg_lines(msgs, 0), msg_lines(msgs, 1), side_lines(cors), at, kb, pair, odd, lats, width)
            for r, m, c in zip(halo, msgs, cors):
                load_row(u, tabs[0][1][("u", 0, r)], m, c(0, 16), lats)
            where = Where()
            for ref, table in zip(before, earlier):
                where.add(ref, table)
            for ref, (_, table) in zip(outs, tabs):
                where.add(ref, table)
            faces(where, rows, fe_rows, width)

        return kernel

    kb_a, kb_b = tabs_a[1][1], tabs_b[1][1]
    fe_tab_a, fe_tab_b = tabs_a[5][1], tabs_b[5][1]
    set_b = call(
        setup_halo(tabs_b, (kb_a, fe_tab_a), halo_b, rows_b, fe_b),
        (near_1, near_2, set_a[1], set_a[5]),
        shapes(tabs_b),
        [],
        "near",
    )
    set_c = call(
        setup_halo(tabs_c, (kb_b, fe_tab_b), halo_c, rows_c, fe_c, True),
        (far_1, far_2, set_b[1], set_b[5]),
        [shapes(tabs_c)[i] for i in (0, 2, 3, 4, 5, 6)],
        [pltpu.VMEM(shapes(tabs_c)[1].shape, F32)],
        "far",
    )

    done_b = [r for s, a, b in todo_b if s == STEPS for r in a + b]
    scratch = [pltpu.VMEM((2, 2, width, 128), F32)] * 2

    def flops(todo):
        return sum(len(a + b) for _, a, b in todo) * width * 1536 * 256 * 2

    def stage(todo, at, final):
        blocks = blocks_of(todo)

        def kernel(tables, n_in, *refs):
            ins, (wh_ref, wl_ref), rest = refs[:n_in], refs[n_in : n_in + 2], refs[n_in + 2 :]
            where = Where()
            for ref, table in zip(ins, tables):
                where.add(ref, table)
            levels, v, vl = rest[0], rest[-2], rest[-1]
            where.add(levels, at)

            def emit(s, r, j, x):
                if s == STEPS:
                    low, high = max(j, PAD), min(j + x.shape[0], PAD + lats)
                    ref, i = final(rest, r)
                    ref[i, low - PAD : high - PAD] = x[low - j : high - j]
                else:
                    levels[pl.ds(at[("u", s, r)] + j, x.shape[0]), :] = x

            cut = pieces(width)

            def run(*flat_accs):
                n = len(cut)
                groups = [flat_accs[i * n : (i + 1) * n] for i in range(4)]
                advance(where, blocks, width, wh_ref, wl_ref, v, vl, emit, (groups[:2], groups[2:]))

            pl.run_scoped(run, *[pltpu.ACC(q)((m, 256), F32) for q in (0, 0, 1, 1) for _, m in cut])

        return kernel

    def used(tabs):
        return [i for i in range(len(tabs)) if i != 1]

    keys_a, keys_b, keys_c = later(todo_a, 99), later(todo_b, STEPS), later(todo_c, STEPS)
    at_a, at_b, at_c = (place(k, width) for k in (keys_a, keys_b, keys_c))

    ins_a = [set_a[i] for i in used(tabs_a)]
    tables_a = [tabs_a[i][1] for i in used(tabs_a)]
    kernel_a = stage(todo_a, at_a, None)
    (lev_a,) = call(
        lambda *refs: kernel_a(tables_a, len(ins_a), *refs),
        (*ins_a, wh, wl),
        [flat(len(keys_a))],
        scratch,
        "inner",
        flops(todo_a),
    )

    def final_b(rest, r):
        return rest[1], done_b.index(r)

    ins_b = ins_a + [lev_a] + [set_b[i] for i in used(tabs_b)]
    tables_b = tables_a + [at_a] + [tabs_b[i][1] for i in used(tabs_b)]
    kernel_b = stage(todo_b, at_b, final_b)
    lev_b, done = call(
        lambda *refs: kernel_b(tables_b, len(ins_b), *refs),
        (*ins_b, wh, wl),
        [flat(len(keys_b)), arr(len(done_b), lats, lev)],
        scratch,
        "middle",
        flops(todo_b),
    )

    def final_c(rest, r):
        return rest[2], r

    ins_c = ins_b + [lev_b] + list(set_c)
    tables_c = tables_b + [at_b] + [tabs_c[i][1] for i in used(tabs_c)]
    kernel_c = stage(todo_c, at_c, final_c)

    def outer(*refs):
        n = len(ins_c) + 2
        done_ref, out, levels, v, vl = refs[n:]
        for i, r in enumerate(done_b):
            out[r] = done_ref[i]
        kernel_c(tables_c, len(ins_c), *refs[:n], levels, done_ref, out, v, vl)

    c_levels = flat(len(keys_c))
    (out,) = call(
        outer,
        (*ins_c, wh, wl, done),
        [arr(*field.shape)],
        [pltpu.VMEM(c_levels.shape, F32)] + scratch,
        "outer",
        flops(todo_c),
        16 << 20,
    )
    return out


def solution(mesh):
    return jax.shard_map(
        body,
        mesh=mesh,
        in_specs=(P("lon", "lat", None), P("lon", "lat"), P("lon", "lat"), P()),
        out_specs=P("lon", "lat", None),
        check_vma=False,
    )
```
